32 devices in a mesh: row: 8 (over z, x), col: 4 (over y, core).
Axes of the slice: x: 2, y: 2, z: 4, core: 2. Of those that a mesh axis runs over, the one named last changes fastest.
Arguments:
- normal_matrix: float32 [4096, 4096], P('row', 'col'), as said below
Outputs:
- factored: float32 [4096, 4096], P('row', 'col')
- log_det: float32 [], replicated
Inputs may be any that keep to these rules, and one draw needn't show every extreme that they name: normal_matrix is symmetric and positive definite.
All inputs are finite; a program needn't handle non-finite values.
Results may differ from the reference program's by a relative error of at most 0.0001.
Values sent between devices are 32-bit elements; how exact they have to be, the bound alone decides.
A program may use at most 64 MiB of HBM per device.

```python
import math
import jax
import jax.numpy as jnp
from jax import lax

B = 512
STEPS = 1
N = 4096


def draw_normal_matrix(key, part):
    key_green = jax.random.fold_in(key, 21)
    key_diag = jax.random.fold_in(key, 22)
    key_scale = jax.random.fold_in(key, 23)
    key_weight = jax.random.fold_in(key, 24)
    observe = 2 * B
    position = jnp.arange(N, dtype=jnp.float32) / N
    rising = jnp.exp(position * math.log(3.0))
    green = jax.random.normal(key_green, (observe, N), jnp.float32)
    data_weight = jnp.exp(jax.random.uniform(key_weight, (observe,), jnp.float32, math.log(0.7), math.log(1.4)))
    diag_add = jax.random.uniform(key_diag, (N,), jnp.float32, 0.5, 2.5)
    rough = jnp.exp(jax.random.uniform(key_scale, (N,), jnp.float32, 0.0, math.log(2.0)))
    scales = 0.6 * rising * rough
    weighted = green * (data_weight / math.sqrt(observe))[:, None]
    gram = jnp.dot(weighted.T, weighted, precision=lax.Precision.HIGHEST)
    base = 0.5 * (gram + gram.T) + jnp.diag(diag_add)
    return base * (scales[:, None] * scales[None, :])


def setup_inputs(seed: int = 0) -> dict:
    key_of = jax.random.split(jax.random.key(seed), 2)
    return {
        "normal_matrix": draw_normal_matrix(jax.random.fold_in(key_of[1], 71), 0),
    }


def reference(normal_matrix):
    matrix = normal_matrix
    log_det = jnp.float32(0.0)
    for panel_step in range(STEPS):
        start_at = panel_step * B
        end_at = start_at + B
        factor = jnp.linalg.cholesky(matrix[start_at:end_at, start_at:end_at])
        panel_cols = jax.scipy.linalg.solve_triangular(factor, matrix[end_at:, start_at:end_at].T, lower=True).T
        update = jnp.dot(panel_cols, panel_cols.T, precision=lax.Precision.HIGHEST)
        matrix = matrix.at[end_at:, end_at:].add(-update)
        matrix = matrix.at[end_at:, start_at:end_at].set(panel_cols)
        matrix = matrix.at[start_at:end_at, start_at:end_at].set(factor)
        matrix = matrix.at[start_at:end_at, end_at:].set(jnp.float32(0.0))
        log_det = log_det + 2.0 * jnp.sum(jnp.log(jnp.diagonal(factor)))
    return (matrix, log_det)
```

```python
import functools

import jax
import jax.numpy as jnp
from jax import lax
from jax.experimental import pallas as pl
from jax.experimental.pallas import tpu as pltpu
from jax.sharding import PartitionSpec as P

MESH = pl.DeviceIdType.MESH
NB = 128
CHUNKS = 4
VMEM = pl.BlockSpec(memory_space=pltpu.VMEM)


def dot_nt(a, b):
    return lax.dot_general(
        a, b, (((1,), (1,)), ((), ())), precision=lax.Precision.HIGHEST,
        preferred_element_type=jnp.float32,
    )


def dot_nn(a, b):
    return lax.dot_general(
        a, b, (((1,), (0,)), ((), ())), precision=lax.Precision.HIGHEST,
        preferred_element_type=jnp.float32,
    )


def factor_block(a):
    groups = NB // 8
    lane = lax.broadcasted_iota(jnp.int32, (8, NB), 1)
    sub = lax.broadcasted_iota(jnp.int32, (8, NB), 0)
    left = [a[8 * g : 8 * g + 8, :] for g in range(groups)]
    right = [(lane == sub + 8 * g).astype(jnp.float32) for g in range(groups)]
    upper, inverse, pivots = [], [], []

    def row(x, t):
        return jnp.broadcast_to(x[t : t + 1, :], (8, NB))

    def column(x, t):
        return jnp.broadcast_to(x[:, t : t + 1], (8, NB))

    for p in range(groups):
        first = 8 * p
        v, i = left[p], right[p]
        cols = [column(v, first + t) for t in range(8)]
        mult = {g: [column(left[g], first + t) for t in range(8)] for g in range(p + 1, groups)}
        u_rows, i_rows, d_rows = v, i, cols[0]
        for t in range(8):
            here = sub == t
            pivot = row(cols[t], t)
            if t:
                u_rows = jnp.where(here, v, u_rows)
                i_rows = jnp.where(here, i, i_rows)
            d_rows = jnp.where(here, pivot, d_rows)
            recip = 1.0 / pivot
            factor = jnp.where(here, -recip, cols[t] * recip)
            for u in range(t + 1, 8):
                cols[u] = jnp.where(here, 0.0, cols[u]) - factor * row(cols[u], t)
            v = jnp.where(here, 0.0, v) - factor * row(v, t)
            i = jnp.where(here, 0.0, i) - factor * row(i, t)
        scale = lax.rsqrt(d_rows)
        upper.append(jnp.where(lane >= sub + first, u_rows * scale, 0.0))
        inverse.append(i_rows * scale)
        pivots.append(d_rows)
        v_rows = [row(v, t) for t in range(8)]
        i_rows = [row(i, t) for t in range(8)]
        for g in range(p + 1, groups):
            left_sum = mult[g][0] * v_rows[0]
            right_sum = mult[g][0] * i_rows[0]
            for t in range(1, 8):
                left_sum = left_sum + mult[g][t] * v_rows[t]
                right_sum = right_sum + mult[g][t] * i_rows[t]
            left[g] = left[g] - left_sum
            right[g] = right[g] - right_sum
    return jnp.concatenate(upper, 0), jnp.concatenate(inverse, 0), jnp.concatenate(pivots, 0)


def cholesky_kernel(a_ref, l_ref, w_ref, logdet_ref, work, upper, inverse, pivot):
    size = a_ref.shape[0]
    work[...] = a_ref[...]
    l_ref[...] = jnp.zeros_like(l_ref)
    w_ref[...] = jnp.zeros_like(w_ref)

    @pl.loop(0, size // NB)
    def _(step):
        span = pl.ds(pl.multiple_of(step * NB, NB), NB)
        r, w, d = factor_block(work[span, span])
        upper[...] = r
        inverse[...] = w
        pivot[span, :] = d
        w_ref[span, span] = inverse[...]
        l_ref[span, span] = upper[...].T
        for p in range(size // NB):

            @pl.when(step == p)
            def _():
                at = slice(p * NB, (p + 1) * NB)
                end = (p + 1) * NB
                if p:
                    inner = dot_nn(l_ref[at, : p * NB], w_ref[: p * NB, : p * NB])
                    w_ref[at, : p * NB] = -dot_nn(inverse[...], inner)
                if end < size:
                    panel = dot_nt(work[end:, at], inverse[...])
                    l_ref[end:, at] = panel
                    work[end:, end:] = work[end:, end:] - dot_nt(panel, panel)

    logdet_ref[...] = jnp.sum(jnp.log(pivot[...]), axis=0, keepdims=True)


def cholesky(a):
    size = a.shape[0]
    square = jax.ShapeDtypeStruct((size, size), jnp.float32)
    return pl.pallas_call(
        cholesky_kernel,
        out_shape=(square, square, jax.ShapeDtypeStruct((1, NB), jnp.float32)),
        in_specs=[VMEM],
        out_specs=(VMEM, VMEM, VMEM),
        scratch_shapes=[
            pltpu.VMEM((size, size), jnp.float32),
            pltpu.VMEM((NB, NB), jnp.float32),
            pltpu.VMEM((NB, NB), jnp.float32),
            pltpu.VMEM((size, NB), jnp.float32),
        ],
    )(a)


def update_kernel(mine_ref, own_ref, cols_ref, w_ref, l_ref, out_ref):
    r, c = lax.axis_index("row"), lax.axis_index("col")
    width = own_ref.shape[0]

    @pl.when(r == 0)
    def _():
        out_ref[...] = jnp.zeros_like(out_ref)

        @pl.when(c == 0)
        def _():
            out_ref[:, :width] = l_ref[...]

    @pl.when(r > 0)
    def _():
        panel = dot_nt(own_ref[...], w_ref[...])
        for slot in range(2):
            at = slice(slot * width, (slot + 1) * width)
            other = dot_nt(cols_ref[at, :], w_ref[...])
            out_ref[:, at] = mine_ref[:, at] - dot_nt(panel, other)

        @pl.when(c == 0)
        def _():
            out_ref[:, :width] = panel


def gather_kernel(mine_ref, own_ref, diag_ref, cols_ref, load_sem, own_send, own_recv,
                  diag_send, diag_recv, cols_send, cols_recv, keep_sem):
    rows, columns = lax.axis_size("row"), lax.axis_size("col")
    r, c = lax.axis_index("row"), lax.axis_index("col")
    q, x = r // 2, r % 2
    other = r + 1 - 2 * x
    width = own_ref.shape[0]
    piece = width // CHUNKS
    even = c % 2 == 0

    links = [
        ((r, c - 1), c >= 1), ((r, c + 1), c + 1 < columns),
        ((r, c - 2), c >= 2), ((r, c + 2), c + 2 < columns),
        ((r - 2, c), r >= 2), ((r + 2, c), r + 2 < rows),
        ((other, c), other >= 0),
    ]
    barrier = pltpu.get_barrier_semaphore()
    for device, exists in links:
        @pl.when(exists)
        def _():
            pl.semaphore_signal(barrier, inc=1, device_id=device, device_id_type=MESH)
    peers = sum(jnp.where(exists, 1, 0).astype(jnp.int32) for _, exists in links)
    pl.semaphore_wait(barrier, peers)

    def part(ref, i, base=0):
        return ref.at[pl.ds(base + i * piece, piece), :]

    def send(source, target, send_sem, recv_sem, device):
        return pltpu.make_async_remote_copy(
            src_ref=source, dst_ref=target, send_sem=send_sem, recv_sem=recv_sem,
            device_id=device, device_id_type=MESH,
        )

    def load(i):
        return pltpu.make_async_copy(
            mine_ref.at[pl.ds(i * piece, piece), pl.ds(0, width)], part(own_ref, i), load_sem.at[i]
        )

    base_x = pl.multiple_of(x * width, width)
    base_o = pl.multiple_of((1 - x) * width, width)
    sends = []

    def forward(condition, *args):
        copy = send(*args)
        sends.append((condition, copy))

        @pl.when(condition)
        def _():
            copy.start()

    def own_part(i):
        return send(part(own_ref, i), part(own_ref, i), own_send.at[0, i], own_recv.at[i], (r, c + 1))

    @pl.when(c == 0)
    def _():
        for i in range(CHUNKS):
            load(i).start()

    keeps = []
    for i in range(CHUNKS):
        @pl.when(c == 0)
        def _():
            load(i).wait()

        @pl.when(c > 0)
        def _():
            own_part(i).wait_recv()

        piece_ref = part(own_ref, i)
        forward(even & (c + 2 < columns), piece_ref, piece_ref, own_send.at[0, i], own_recv.at[i], (r, c + 2))
        forward(even, piece_ref, piece_ref, own_send.at[1, i], own_recv.at[i], (r, c + 1))
        forward((r == 0) & even & (rows > 2), piece_ref, part(diag_ref, i), diag_send.at[0, i], diag_recv.at[i], (r + 2, c))
        forward((r == 0) & even, piece_ref, part(diag_ref, i), diag_send.at[1, i], diag_recv.at[i], (r + 1, c))
        keep = pltpu.make_async_copy(piece_ref, part(diag_ref, i), keep_sem.at[0, i])
        keeps.append((r == 0, keep))

        @pl.when(r == 0)
        def _():
            keep.start()

    for i in range(CHUNKS):
        diag_piece = part(diag_ref, i)
        incoming = send(diag_piece, diag_piece, diag_send.at[0, i], diag_recv.at[i], (other, c))

        @pl.when(r > 0)
        def _():
            incoming.wait_recv()

        forward((r > 0) & even & (x == 0) & (r + 2 < rows), diag_piece, diag_piece, diag_send.at[0, i], diag_recv.at[i], (r + 2, c))
        forward((r > 0) & even & (x == 0), diag_piece, diag_piece, diag_send.at[1, i], diag_recv.at[i], (r + 1, c))
        forward((r > 0) & even, diag_piece, diag_piece, diag_send.at[2, i], diag_recv.at[i], (r, c + 1))

    for i in range(CHUNKS):
        target = part(cols_ref, i, base_x)

        def spread(condition, source):
            forward(condition & (q >= c) & (r + 2 < rows), source, target, cols_send.at[0, i], cols_recv.at[0, i], (r + 2, c))
            forward(condition & (q <= c) & (q > 0), source, target, cols_send.at[1, i], cols_recv.at[0, i], (r - 2, c))
            forward(condition, source, target, cols_send.at[2, i], cols_recv.at[1, i], (other, c))

        keep = pltpu.make_async_copy(part(own_ref, i), target, keep_sem.at[1, i])
        keeps.append((q == c, keep))

        @pl.when(q == c)
        def _():
            keep.start()

        spread(q == c, part(own_ref, i))
        incoming = send(target, target, cols_send.at[0, i], cols_recv.at[0, i], (other, c))

        @pl.when(q != c)
        def _():
            incoming.wait_recv()

        spread(q != c, target)

    for i in range(CHUNKS):
        target = part(cols_ref, i, base_o)
        send(target, target, cols_send.at[2, i], cols_recv.at[1, i], (other, c)).wait_recv()
    for condition, copy in sends:
        @pl.when(condition)
        def _():
            copy.wait_send()
    for condition, copy in keeps:
        @pl.when(condition)
        def _():
            copy.wait()


def gather(mine):
    width = mine.shape[0]
    square = jax.ShapeDtypeStruct((width, width), jnp.float32)
    dma = pltpu.SemaphoreType.DMA
    return pl.pallas_call(
        gather_kernel,
        out_shape=(square, square, jax.ShapeDtypeStruct((2 * width, width), jnp.float32)),
        in_specs=[pl.BlockSpec(memory_space=pl.ANY)],
        out_specs=(VMEM, VMEM, VMEM),
        scratch_shapes=[
            dma((CHUNKS,)), dma((2, CHUNKS)), dma((CHUNKS,)), dma((3, CHUNKS)), dma((CHUNKS,)),
            dma((3, CHUNKS)), dma((2, CHUNKS)), dma((2, CHUNKS)),
        ],
        compiler_params=pltpu.CompilerParams(collective_id=0, has_side_effects=True),
    )(mine)


def per_device(mine):
    own, diag, cols = gather(mine)
    l, w, logdet = cholesky(diag)
    block = pl.pallas_call(
        update_kernel,
        out_shape=jax.ShapeDtypeStruct(mine.shape, jnp.float32),
        in_specs=[VMEM] * 5,
        out_specs=VMEM,
    )(mine, own, cols, w, l)
    return block, logdet[0, 0]


def solution(mesh):
    return jax.shard_map(
        per_device, mesh=mesh, in_specs=(P("row", "col"),), out_specs=(P("row", "col"), P()), check_vma=False
    )
```

```python
import functools

import jax
import jax.numpy as jnp
from jax import lax
from jax.experimental import pallas as pl
from jax.experimental.pallas import tpu as pltpu
from jax.sharding import PartitionSpec as P

MESH = pl.DeviceIdType.MESH
NB = 128
CHUNKS = 8
VMEM = pl.BlockSpec(memory_space=pltpu.VMEM)


def dot_nt(a, b):
    return lax.dot_general(
        a, b, (((1,), (1,)), ((), ())), precision=lax.Precision.HIGHEST,
        preferred_element_type=jnp.float32,
    )


def dot_nn(a, b):
    return lax.dot_general(
        a, b, (((1,), (0,)), ((), ())), precision=lax.Precision.HIGHEST,
        preferred_element_type=jnp.float32,
    )


def split(a):
    high = a.astype(jnp.bfloat16)
    return high, (a - high.astype(jnp.float32)).astype(jnp.bfloat16)


def dot_nt_split(a, b):
    def dot(u, v):
        return lax.dot_general(u, v, (((1,), (1,)), ((), ())), preferred_element_type=jnp.float32)

    return dot(a[0], b[0]) + (dot(a[0], b[1]) + dot(a[1], b[0]))


def solve(rows, w_ref):
    size = w_ref.shape[0]
    half = size // 2
    return jnp.concatenate(
        [dot_nt(rows[:, : e], w_ref[e - half : e, :e]) for e in range(half, size + 1, half)], axis=1
    )


def factor_block(a, hook):
    groups = NB // 8
    lane = lax.broadcasted_iota(jnp.int32, (8, NB), 1)
    sub = lax.broadcasted_iota(jnp.int32, (8, NB), 0)
    left = [a[8 * g : 8 * g + 8, :] for g in range(groups)]
    right = [(lane == sub + 8 * g).astype(jnp.float32) for g in range(groups)]
    upper, inverse, pivots = [], [], []

    def row(x, t):
        return jnp.broadcast_to(x[t : t + 1, :], (8, NB))

    def column(x, t):
        return jnp.broadcast_to(x[:, t : t + 1], (8, NB))

    for p in range(groups):
        if p == groups // 2:
            hook()
        first = 8 * p
        v, i = left[p], right[p]
        cols = [column(v, first + t) for t in range(8)]
        mult = {g: [column(left[g], first + t) for t in range(8)] for g in range(p + 1, groups)}
        u_rows, i_rows, d_rows = v, i, cols[0]
        for t in range(8):
            here = sub == t
            pivot = row(cols[t], t)
            if t:
                u_rows = jnp.where(here, v, u_rows)
                i_rows = jnp.where(here, i, i_rows)
            d_rows = jnp.where(here, pivot, d_rows)
            recip = 1.0 / pivot
            factor = jnp.where(here, -recip, cols[t] * recip)
            for u in range(t + 1, 8):
                cols[u] = jnp.where(here, 0.0, cols[u]) - factor * row(cols[u], t)
            v = jnp.where(here, 0.0, v) - factor * row(v, t)
            i = jnp.where(here, 0.0, i) - factor * row(i, t)
        scale = lax.rsqrt(d_rows)
        upper.append(jnp.where(lane >= sub + first, u_rows * scale, 0.0))
        inverse.append(i_rows * scale)
        pivots.append(d_rows)
        v_rows = [row(v, t) for t in range(8)]
        i_rows = [row(i, t) for t in range(8)]
        for g in range(p + 1, groups):
            left_sum = mult[g][0] * v_rows[0]
            right_sum = mult[g][0] * i_rows[0]
            for t in range(1, 8):
                left_sum = left_sum + mult[g][t] * v_rows[t]
                right_sum = right_sum + mult[g][t] * i_rows[t]
            left[g] = left[g] - left_sum
            right[g] = right[g] - right_sum
    return jnp.concatenate(upper, 0), jnp.concatenate(inverse, 0), jnp.concatenate(pivots, 0)


def factor_all(a_ref, l_ref, w_ref, logdet_ref, work, upper, inverse, pivot, relay):
    size = a_ref.shape[0]
    for end in range(NB, size + 1, NB):
        work[end - NB : end, :end] = a_ref[end - NB : end, :end]
    l_ref[...] = jnp.zeros_like(l_ref)
    w_ref[...] = jnp.zeros_like(w_ref)

    @pl.loop(0, size // NB)
    def _(step):
        span = pl.ds(pl.multiple_of(step * NB, NB), NB)
        r, w, d = factor_block(work[span, span], lambda: relay(2 * step))
        upper[...] = r
        inverse[...] = w
        pivot[span, :] = d
        w_ref[span, span] = inverse[...]
        l_ref[span, span] = upper[...].T
        relay(2 * step + 1)
        for p in range(size // NB):

            @pl.when(step == p)
            def _():
                at = slice(p * NB, (p + 1) * NB)
                end = (p + 1) * NB
                if p:
                    inner = dot_nn(l_ref[at, : p * NB], w_ref[: p * NB, : p * NB])
                    w_ref[at, : p * NB] = -dot_nn(inverse[...], inner)
                if end < size:
                    panel = dot_nt(work[end:, at], inverse[...])
                    l_ref[end:, at] = panel
                    for col in range(end, size, NB):
                        block = panel[col - end : col - end + NB, :]
                        work[col:, col : col + NB] = work[col:, col : col + NB] - dot_nt(panel[col - end :, :], block)

    logdet_ref[...] = jnp.sum(jnp.log(pivot[...]), axis=0, keepdims=True)


def update_kernel(mine_ref, own_ref, cols_ref, w_ref, l_ref, out_ref):
    r, c = lax.axis_index("row"), lax.axis_index("col")
    width = own_ref.shape[0]

    @pl.when(r == 0)
    def _():
        out_ref[...] = jnp.zeros_like(out_ref)

        @pl.when(c == 0)
        def _():
            out_ref[:, :width] = l_ref[...]

    @pl.when(r > 0)
    def _():
        panel = solve(own_ref[...], w_ref)
        panel_split = split(panel)
        for slot in range(2):
            at = slice(slot * width, (slot + 1) * width)
            other = solve(cols_ref[at, :], w_ref)
            out_ref[:, at] = mine_ref[:, at] - dot_nt_split(panel_split, split(other))

        @pl.when(c == 0)
        def _():
            out_ref[:, :width] = panel


def panel_kernel(mine_ref, own_ref, cols_ref, l_ref, w_ref, logdet_ref, diag_ref, work, upper, inverse, pivot,
                 load_sem, own_send, own_recv, diag_send, diag_recv, cols_send, cols_recv, keep_sem):
    rows, columns = lax.axis_size("row"), lax.axis_size("col")
    r, c = lax.axis_index("row"), lax.axis_index("col")
    q, x = r // 2, r % 2
    other = r + 1 - 2 * x
    width = own_ref.shape[0]
    piece = width // CHUNKS
    even = c % 2 == 0

    links = [
        ((r, c - 1), c >= 1), ((r, c + 1), c + 1 < columns),
        ((r, c - 2), c >= 2), ((r, c + 2), c + 2 < columns),
        ((r - 2, c), r >= 2), ((r + 2, c), r + 2 < rows),
        ((other, c), other >= 0),
    ]
    barrier = pltpu.get_barrier_semaphore()
    for device, exists in links:
        @pl.when(exists)
        def _():
            pl.semaphore_signal(barrier, inc=1, device_id=device, device_id_type=MESH)
    peers = sum(jnp.where(exists, 1, 0).astype(jnp.int32) for _, exists in links)
    pl.semaphore_wait(barrier, peers)

    def part(ref, i, base=0):
        return ref.at[pl.ds(pl.multiple_of(base + i * piece, piece), piece), :]

    def low(ref, i):
        seen = -(-((i + 1) * piece) // NB) * NB
        return ref.at[pl.ds(i * piece, piece), pl.ds(0, seen)]

    def send(source, target, send_sem, recv_sem, device):
        return pltpu.make_async_remote_copy(
            src_ref=source, dst_ref=target, send_sem=send_sem, recv_sem=recv_sem,
            device_id=device, device_id_type=MESH,
        )

    def load(i):
        return pltpu.make_async_copy(
            mine_ref.at[pl.ds(i * piece, piece), pl.ds(0, width)], part(own_ref, i), load_sem.at[i]
        )

    base_x = pl.multiple_of(x * width, width)
    base_o = pl.multiple_of((1 - x) * width, width)
    sends = []

    def forward(condition, *args):
        copy = send(*args)
        sends.append((condition, copy))

        @pl.when(condition)
        def _():
            copy.start()

    def spread(i, source):
        target = part(cols_ref, i, base_x)
        return [
            ((q >= c) & (r + 2 < rows), send(source, target, cols_send.at[0, i], cols_recv.at[0, i], (r + 2, c))),
            ((q <= c) & (q > 0), send(source, target, cols_send.at[1, i], cols_recv.at[0, i], (r - 2, c))),
            (q >= 0, send(source, target, cols_send.at[2, i], cols_recv.at[1, i], (other, c))),
        ]

    def start(condition, copies):
        for exists, copy in copies:
            @pl.when(condition & exists)
            def _():
                copy.start()

    def relay(i):
        target = part(cols_ref, i, base_x)

        @pl.when(q != c)
        def _():
            send(target, target, cols_send.at[0, i], cols_recv.at[0, i], (other, c)).wait_recv()

        start(q != c, spread(i, target))

    def own_part(i):
        return send(part(own_ref, i), part(own_ref, i), own_send.at[0, i], own_recv.at[i], (r, c + 1))

    @pl.when(c == 0)
    def _():
        for i in range(CHUNKS):
            load(i).start()

    keeps = []
    for i in range(CHUNKS):
        @pl.when(c == 0)
        def _():
            load(i).wait()

        @pl.when(c > 0)
        def _():
            own_part(i).wait_recv()

        piece_ref = part(own_ref, i)
        forward(even & (c + 2 < columns), piece_ref, piece_ref, own_send.at[0, i], own_recv.at[i], (r, c + 2))
        forward(even, piece_ref, piece_ref, own_send.at[1, i], own_recv.at[i], (r, c + 1))
        low_ref = low(own_ref, i)
        forward((r == 0) & even & (rows > 2), low_ref, low(diag_ref, i), diag_send.at[0, i], diag_recv.at[i], (r + 2, c))
        forward((r == 0) & even, low_ref, low(diag_ref, i), diag_send.at[1, i], diag_recv.at[i], (r + 1, c))
        keep = pltpu.make_async_copy(low_ref, low(diag_ref, i), keep_sem.at[0, i])

        @pl.when(r == 0)
        def _():
            keep.start()

        start(q == c, spread(i, piece_ref))
        keep_cols = pltpu.make_async_copy(piece_ref, part(cols_ref, i, base_x), keep_sem.at[1, i])
        keeps.append((q == c, keep_cols))

        @pl.when(q == c)
        def _():
            keep_cols.start()

    for i in range(CHUNKS):
        diag_piece = low(diag_ref, i)
        incoming = send(diag_piece, diag_piece, diag_send.at[0, i], diag_recv.at[i], (other, c))

        @pl.when(r > 0)
        def _():
            incoming.wait_recv()

        forward((r > 0) & even & (x == 0) & (r + 2 < rows), diag_piece, diag_piece, diag_send.at[0, i], diag_recv.at[i], (r + 2, c))
        forward((r > 0) & even & (x == 0), diag_piece, diag_piece, diag_send.at[1, i], diag_recv.at[i], (r + 1, c))
        forward((r > 0) & even, diag_piece, diag_piece, diag_send.at[2, i], diag_recv.at[i], (r, c + 1))

    for i in range(CHUNKS):
        @pl.when(r == 0)
        def _():
            pltpu.make_async_copy(low(own_ref, i), low(diag_ref, i), keep_sem.at[0, i]).wait()

    factor_all(diag_ref, l_ref, w_ref, logdet_ref, work, upper, inverse, pivot, relay)

    for i in range(CHUNKS):
        target = part(cols_ref, i, base_o)
        send(target, target, cols_send.at[2, i], cols_recv.at[1, i], (other, c)).wait_recv()
    for i in range(CHUNKS):
        sends += spread(i, part(cols_ref, i, base_x))
    for condition, copy in sends:
        @pl.when(condition)
        def _():
            copy.wait_send()
    for condition, copy in keeps:
        @pl.when(condition)
        def _():
            copy.wait()


def panel_step(mine):
    width = mine.shape[0]
    square = jax.ShapeDtypeStruct((width, width), jnp.float32)
    dma = pltpu.SemaphoreType.DMA
    return pl.pallas_call(
        panel_kernel,
        out_shape=(
            square, jax.ShapeDtypeStruct((2 * width, width), jnp.float32), square, square,
            jax.ShapeDtypeStruct((1, NB), jnp.float32),
        ),
        in_specs=[pl.BlockSpec(memory_space=pl.ANY)],
        out_specs=(VMEM,) * 5,
        scratch_shapes=[
            pltpu.VMEM((width, width), jnp.float32), pltpu.VMEM((width, width), jnp.float32),
            pltpu.VMEM((NB, NB), jnp.float32), pltpu.VMEM((NB, NB), jnp.float32),
            pltpu.VMEM((width, NB), jnp.float32),
            dma((CHUNKS,)), dma((2, CHUNKS)), dma((CHUNKS,)), dma((3, CHUNKS)), dma((CHUNKS,)),
            dma((3, CHUNKS)), dma((2, CHUNKS)), dma((2, CHUNKS)),
        ],
        compiler_params=pltpu.CompilerParams(collective_id=0, has_side_effects=True),
    )(mine)


def per_device(mine):
    own, cols, l, w, logdet = panel_step(mine)
    block = pl.pallas_call(
        update_kernel,
        out_shape=jax.ShapeDtypeStruct(mine.shape, jnp.float32),
        in_specs=[VMEM] * 5,
        out_specs=VMEM,
    )(mine, own, cols, w, l)
    return block, logdet[0, 0]


def solution(mesh):
    return jax.shard_map(
        per_device, mesh=mesh, in_specs=(P("row", "col"),), out_specs=(P("row", "col"), P()), check_vma=False
    )
```
